8 devices in a mesh: dp: 2 (over z, y), pp: 4 (over x, core).
Axes of the slice: x: 2, y: 2, z: 1, core: 2. Of those that a mesh axis runs over, the one named last changes fastest.
Arguments:
- x_in: bfloat16 [8, 2, 1024, 768], P(('dp', 'pp')), parts along dimension 0
- dy_out: bfloat16 [8, 2, 1024, 768], P(('dp', 'pp')), parts along dimension 0
- w_qkv: bfloat16 [4, 2, 1, 768, 3, 12, 64], P('pp')
- w_attn: bfloat16 [4, 2, 1, 12, 64, 768], P('pp')
- w_fc: bfloat16 [4, 2, 1, 768, 3072], P('pp')
- w_proj: bfloat16 [4, 2, 1, 3072, 768], P('pp')
- b_qkv: bfloat16 [4, 2, 1, 3, 12, 64], P('pp')
- b_fc: bfloat16 [4, 2, 1, 3072], P('pp')
- vec_d: bfloat16 [4, 2, 1, 6, 768], P('pp')
Outputs:
- output 1: bfloat16 [8, 2, 1024, 768], P(('dp', 'pp')), parts along dimension 0
- output 2: bfloat16 [8, 2, 1024, 768], P(('dp', 'pp')), parts along dimension 0
- output 3: float32 [8, 2, 1, 768, 3, 12, 64], P(('dp', 'pp')), parts along dimension 0
- output 4: float32 [8, 2, 1, 12, 64, 768], P(('dp', 'pp')), parts along dimension 0
- output 5: float32 [8, 2, 1, 768, 3072], P(('dp', 'pp')), parts along dimension 0
- output 6: float32 [8, 2, 1, 3072, 768], P(('dp', 'pp')), parts along dimension 0
- output 7: float32 [8, 2, 1, 3, 12, 64], P(('dp', 'pp')), parts along dimension 0
- output 8: float32 [8, 2, 1, 3072], P(('dp', 'pp')), parts along dimension 0
- output 9: float32 [8, 2, 1, 6, 768], P(('dp', 'pp')), parts along dimension 0
There are 2 independent parts. The reference program is written for one: setup_inputs(seed, part) draws one part's arguments, and reference() takes and returns one part's arrays. A program takes and returns all parts, laid end to end along the dimension named above; an argument that names none is the same for every part.
All inputs are finite; a program needn't handle non-finite values.
Results may differ from the reference program's by a relative error of at most 0.0149549.
Values are sent between devices in bfloat16 or wider.
A program may use at most 1 GiB of HBM per device.

```python
import jax
import jax.numpy as jnp
from jax import lax

STAGES = 4
MICRO = 4
LPS = 1
BATCH = 2
SEQ = 1024
DM = 768
HEADS = 12
FF = 3072
HEAD = DM // HEADS
LAYERS = STAGES * LPS
EPSILON = 1e-5


def with_second_copy(stage_major):
    return jnp.stack([stage_major, stage_major[::-1]], axis=1).astype(jnp.bfloat16)


def setup_inputs(seed: int = 0, part: int = 0) -> dict:
    root_key = jax.random.key(seed)
    data_keys = jax.random.split(jax.random.fold_in(root_key, part), 2)
    w_keys = jax.random.split(jax.random.key(seed + 7919), 7)
    res_scale = (2.0 * LAYERS) ** -0.5
    act_shape = (MICRO, BATCH, SEQ, DM)
    x_in = jax.random.normal(data_keys[0], act_shape, jnp.float32).astype(jnp.bfloat16)
    dy_out = jax.random.normal(data_keys[1], act_shape, jnp.float32).astype(jnp.bfloat16)
    w_qkv = with_second_copy(jax.random.normal(w_keys[0], (STAGES, LPS, DM, 3, HEADS, HEAD), jnp.float32) * DM ** -0.5)
    w_attn = with_second_copy(jax.random.normal(w_keys[1], (STAGES, LPS, HEADS, HEAD, DM), jnp.float32) * (DM ** -0.5 * res_scale))
    w_fc = with_second_copy(jax.random.normal(w_keys[2], (STAGES, LPS, DM, FF), jnp.float32) * DM ** -0.5)
    w_proj = with_second_copy(jax.random.normal(w_keys[3], (STAGES, LPS, FF, DM), jnp.float32) * (FF ** -0.5 * res_scale))
    b_qkv = with_second_copy(0.3 * jax.random.normal(w_keys[4], (STAGES, LPS, 3, HEADS, HEAD), jnp.float32))
    b_fc = with_second_copy(0.3 * jax.random.normal(w_keys[5], (STAGES, LPS, FF), jnp.float32))
    row_scale = jnp.array([0.2, 0.2, 0.5 * res_scale, 0.2, 0.2, 0.5 * res_scale], jnp.float32)
    row_shift = jnp.array([1.0, 0.0, 0.0, 1.0, 0.0, 0.0], jnp.float32)
    vec_rows = jax.random.normal(w_keys[6], (STAGES, LPS, 6, DM), jnp.float32)
    vec_d = with_second_copy(vec_rows * row_scale[:, None] + row_shift[:, None])
    return {'x_in': x_in, 'dy_out': dy_out, 'w_qkv': w_qkv, 'w_attn': w_attn, 'w_fc': w_fc, 'w_proj': w_proj, 'b_qkv': b_qkv, 'b_fc': b_fc, 'vec_d': vec_d}


def layer_norm(rows_in, ln_gain, ln_shift):
    rows_f32 = rows_in.astype(jnp.float32)
    row_mean = jnp.mean(rows_f32, axis=-1, keepdims=True)
    centered = rows_f32 - row_mean
    row_var = jnp.mean(centered * centered, axis=-1, keepdims=True)
    scaled = centered * lax.rsqrt(row_var + EPSILON)
    return (scaled * ln_gain.astype(jnp.float32) + ln_shift.astype(jnp.float32)).astype(jnp.bfloat16)


def gpt_layer(hidden_in, layer_w):
    w_qkv, w_attn, w_fc, w_proj, b_qkv, b_fc, vec_d = layer_w
    n_batch, seq_len, d_model = hidden_in.shape
    n_heads, head_dim = w_qkv.shape[-2], w_qkv.shape[-1]
    tokens = n_batch * seq_len
    flat_rows = hidden_in.reshape(tokens, d_model)
    normed = layer_norm(flat_rows, vec_d[0], vec_d[1])
    qkv_proj = jnp.dot(normed, w_qkv.reshape(d_model, 3 * d_model), preferred_element_type=jnp.float32)
    qkv_proj = (qkv_proj + b_qkv.reshape(3 * d_model).astype(jnp.float32)).astype(jnp.bfloat16)
    qkv_proj = qkv_proj.reshape(n_batch, seq_len, 3, n_heads, head_dim)
    query_heads = qkv_proj[:, :, 0].astype(jnp.float32)
    key_heads = qkv_proj[:, :, 1].astype(jnp.float32)
    value_heads = qkv_proj[:, :, 2].astype(jnp.float32)
    scores = jnp.einsum('bqhe,bkhe->bhqk', query_heads, key_heads) * (head_dim ** -0.5)
    causal = jnp.arange(seq_len)[:, None] >= jnp.arange(seq_len)[None, :]
    scores = jnp.where(causal, scores, -1e30)
    attn_probs = jax.nn.softmax(scores, axis=-1).astype(jnp.bfloat16)
    mixed_heads = jnp.einsum('bhqk,bkhe->bqhe', attn_probs.astype(jnp.float32), value_heads).astype(jnp.bfloat16)
    attn_out = jnp.dot(mixed_heads.reshape(tokens, d_model), w_attn.reshape(d_model, d_model), preferred_element_type=jnp.float32)
    residual = (flat_rows.astype(jnp.float32) + attn_out + vec_d[2].astype(jnp.float32)).astype(jnp.bfloat16)
    normed_two = layer_norm(residual, vec_d[3], vec_d[4])
    hidden = jnp.dot(normed_two, w_fc, preferred_element_type=jnp.float32) + b_fc.astype(jnp.float32)
    hidden = jax.nn.gelu(hidden, approximate=True).astype(jnp.bfloat16)
    mlp_out = jnp.dot(hidden, w_proj, preferred_element_type=jnp.float32) + vec_d[5].astype(jnp.float32)
    return (residual.astype(jnp.float32) + mlp_out).astype(jnp.bfloat16).reshape(n_batch, seq_len, d_model)


def stack_forward(hidden_in, layer_ws):
    def scan_body(carry, layer_w):
        return gpt_layer(carry, layer_w), None
    out_h, _ = lax.scan(scan_body, hidden_in, layer_ws)
    return out_h


def copy_pass(x_part, dy_part, layer_ws):
    grad_zero = tuple(jnp.zeros(t.shape, jnp.float32) for t in layer_ws)
    def scan_body(grad_acc, mb_pair):
        x_mb, dy_mb = mb_pair
        y_mb, pull_back = jax.vjp(stack_forward, x_mb, layer_ws)
        dx_mb, dw_mb = pull_back(dy_mb)
        grad_acc = tuple(a + g.astype(jnp.float32) for a, g in zip(grad_acc, dw_mb))
        return grad_acc, (y_mb, dx_mb)
    grad_acc, (y_half, dx_half) = lax.scan(scan_body, grad_zero, (x_part, dy_part))
    return y_half, dx_half, grad_acc


def reference(x_in, dy_out, w_qkv, w_attn, w_fc, w_proj, b_qkv, b_fc, vec_d):
    params = (w_qkv, w_attn, w_fc, w_proj, b_qkv, b_fc, vec_d)
    half_micro = MICRO // 2
    down_ws = tuple(t[:, 0].reshape((LAYERS,) + t.shape[3:]) for t in params)
    up_ws = tuple(t[::-1, 1].reshape((LAYERS,) + t.shape[3:]) for t in params)
    y_down, dx_down, g_down = copy_pass(x_in[:half_micro], dy_out[:half_micro], down_ws)
    y_up, dx_up, g_up = copy_pass(x_in[half_micro:], dy_out[half_micro:], up_ws)
    y_out = jnp.concatenate([y_down, y_up], axis=0)
    dx_in = jnp.concatenate([dx_down, dx_up], axis=0)
    grads = []
    for orig, part_down, part_up in zip(params, g_down, g_up):
        total = (part_down + part_up).reshape((STAGES, LPS) + orig.shape[3:])
        grads.append(jnp.stack([total, total[::-1]], axis=1))
    return (y_out, dx_in, grads[0], grads[1], grads[2], grads[3], grads[4], grads[5], grads[6])
```

```python
import functools

import jax
import jax.numpy as jnp
from jax import lax
from jax.experimental import pallas as pl
from jax.experimental.pallas import tpu as pltpu
from jax.sharding import PartitionSpec as P

EPSILON = 1e-5
HEADS = 12
HEAD = 64
LOG2E = 1.4426950408889634
SCALE = HEAD ** -0.5
BLK = 256
F32 = jnp.float32
BF16 = jnp.bfloat16
NT = (((1,), (1,)), ((), ()))
NN = (((1,), (0,)), ((), ()))
TN = (((0,), (0,)), ((), ()))


def mm(a, b, dims):
    return lax.dot_general(a, b, dims, preferred_element_type=F32)


def attn_fwd_body(q_ref, k_ref, v_ref, o_ref, lse_ref, lse_scr):
    pair = pl.program_id(1)
    seq = q_ref.shape[0]
    n_blk = seq // BLK
    lane = lax.broadcasted_iota(jnp.int32, (BLK, 128), 1)
    causal = lax.broadcasted_iota(jnp.int32, (BLK, BLK), 0) >= lax.broadcasted_iota(jnp.int32, (BLK, BLK), 1)

    @pl.when(pair == 0)
    def _():
        lse_scr[...] = jnp.zeros_like(lse_scr)

    zero = jnp.zeros((BLK, 128), BF16)
    for i in range(n_blk):
        rows = slice(i * BLK, (i + 1) * BLK)
        q_blk = q_ref[rows, :]
        heads_out = []
        stats = lse_scr[rows, :]
        for h in range(2):
            q_h = jnp.where((lane < HEAD) == (h == 0), q_blk, zero)
            s_d = jnp.where(causal, mm(q_h, k_ref[rows, :], NT), -1e30)
            top = jnp.max(s_d, axis=1, keepdims=True)
            if i:
                s_o = mm(q_h, k_ref[: i * BLK, :], NT)
                top = jnp.maximum(top, jnp.max(s_o, axis=1, keepdims=True))
            e_d = jnp.exp2((s_d - top) * (SCALE * LOG2E))
            total = jnp.sum(e_d, axis=1, keepdims=True)
            if i:
                e_o = jnp.exp2((s_o - top) * (SCALE * LOG2E))
                total = total + jnp.sum(e_o, axis=1, keepdims=True)
            inv = 1.0 / total
            out = mm((e_d * inv).astype(BF16), v_ref[rows, :], NN)
            if i:
                out = out + mm((e_o * inv).astype(BF16), v_ref[: i * BLK, :], NN)
            heads_out.append(out)
            stats = jnp.where(lane == 2 * pair + h, top * (SCALE * LOG2E) + jnp.log2(total), stats)
        o_ref[rows, :] = jnp.where(lane < HEAD, heads_out[0], heads_out[1]).astype(BF16)
        lse_scr[rows, :] = stats

    @pl.when(pair == pl.num_programs(1) - 1)
    def _():
        lse_ref[0] = lse_scr[...].T[: lse_ref.shape[1], :]


def attn_fwd(qkv, batch):
    tokens = qkv.shape[0]
    seq = tokens // batch
    width = HEADS * HEAD
    pairs = width // 128
    return pl.pallas_call(
        attn_fwd_body,
        grid=(batch, pairs),
        in_specs=[
            pl.BlockSpec((seq, 128), lambda b, p: (b, p)),
            pl.BlockSpec((seq, 128), lambda b, p: (b, pairs + p)),
            pl.BlockSpec((seq, 128), lambda b, p: (b, 2 * pairs + p)),
        ],
        out_specs=[
            pl.BlockSpec((seq, 128), lambda b, p: (b, p)),
            pl.BlockSpec((1, 16, seq), lambda b, p: (b, 0, 0)),
        ],
        out_shape=[
            jax.ShapeDtypeStruct((tokens, width), BF16),
            jax.ShapeDtypeStruct((batch, 16, seq), F32),
        ],
        scratch_shapes=[pltpu.VMEM((seq, 128), F32)],
        compiler_params=pltpu.CompilerParams(vmem_limit_bytes=48 * 1024 * 1024),
        cost_estimate=pl.CostEstimate(flops=2 * 2 * batch * HEADS * seq * seq * HEAD * 4, bytes_accessed=tokens * width * 8, transcendentals=batch * HEADS * seq * seq // 2),
        name="attn_fwd",
    )(qkv, qkv, qkv)


def attn_bwd_body(q_ref, k_ref, v_ref, do_ref, o_ref, lse_ref, dqkv_ref, dq_scr, delta_scr):
    pair = pl.program_id(1)
    seq = q_ref.shape[0]
    n_blk = seq // BLK
    lane = lax.broadcasted_iota(jnp.int32, (seq, 128), 1)
    first = lane < HEAD
    causal_t = lax.broadcasted_iota(jnp.int32, (BLK, BLK), 0) <= lax.broadcasted_iota(jnp.int32, (BLK, BLK), 1)
    prod = do_ref[...].astype(F32) * o_ref[...].astype(F32)
    d_0 = jnp.sum(jnp.where(first, prod, 0.0), axis=1, keepdims=True)
    d_1 = jnp.sum(jnp.where(first, 0.0, prod), axis=1, keepdims=True)
    delta_scr[...] = jnp.where(lane == 0, d_0, d_1).T[:8, :]
    zero = jnp.zeros((seq, 128), BF16)
    q_h = [jnp.where(first, q_ref[...], zero), jnp.where(first, zero, q_ref[...])]
    do_h = [jnp.where(first, do_ref[...], zero), jnp.where(first, zero, do_ref[...])]
    k_h = [jnp.where(first, k_ref[...], zero), jnp.where(first, zero, k_ref[...])]
    dq_scr[...] = jnp.zeros_like(dq_scr)
    for j in range(n_blk):
        keys = slice(j * BLK, (j + 1) * BLK)
        k_blk, v_blk = k_ref[keys, :], v_ref[keys, :]
        dk = jnp.zeros((BLK, 128), F32)
        dv = jnp.zeros((BLK, 128), F32)
        for h in range(2):
            parts = [(keys, True)]
            if j + 1 < n_blk:
                parts.append((slice((j + 1) * BLK, seq), False))
            for rows, diag in parts:
                q_p, do_p = q_h[h][rows], do_h[h][rows]
                s_t = mm(k_blk, q_p, NT)
                lse = lse_ref[0, pl.ds(2 * pair + h, 1), rows]
                p_t = jnp.exp2(s_t * (SCALE * LOG2E) - lse)
                if diag:
                    p_t = jnp.where(causal_t, p_t, 0.0)
                dp_t = mm(v_blk, do_p, NT)
                ds_t = (p_t * (dp_t - delta_scr[h : h + 1, rows])).astype(BF16)
                dv = dv + mm(p_t.astype(BF16), do_p, NN)
                dk = dk + mm(ds_t, q_p, NN)
                dq_scr[rows, :] += mm(ds_t, k_h[h][keys], TN)
        dqkv_ref[1, keys, :] = (dk * SCALE).astype(BF16)
        dqkv_ref[2, keys, :] = dv.astype(BF16)
    dqkv_ref[0] = (dq_scr[...] * SCALE).astype(BF16)


def attn_bwd(qkv, d_out, out, lse, batch):
    tokens = qkv.shape[0]
    seq = tokens // batch
    width = HEADS * HEAD
    pairs = width // 128
    return pl.pallas_call(
        attn_bwd_body,
        grid=(batch, pairs),
        in_specs=[
            pl.BlockSpec((seq, 128), lambda b, p: (b, p)),
            pl.BlockSpec((seq, 128), lambda b, p: (b, pairs + p)),
            pl.BlockSpec((seq, 128), lambda b, p: (b, 2 * pairs + p)),
            pl.BlockSpec((seq, 128), lambda b, p: (b, p)),
            pl.BlockSpec((seq, 128), lambda b, p: (b, p)),
            pl.BlockSpec((1, 16, seq), lambda b, p: (b, 0, 0)),
        ],
        out_specs=pl.BlockSpec((3, seq, 128), lambda b, p: (0, b, p)),
        out_shape=jax.ShapeDtypeStruct((3, tokens, width), BF16),
        scratch_shapes=[pltpu.VMEM((seq, 128), F32), pltpu.VMEM((8, seq), F32)],
        compiler_params=pltpu.CompilerParams(vmem_limit_bytes=56 * 1024 * 1024),
        cost_estimate=pl.CostEstimate(flops=2 * 5 * batch * HEADS * seq * seq * HEAD * 4, bytes_accessed=tokens * width * 16, transcendentals=batch * HEADS * seq * seq // 2),
        name="attn_bwd",
    )(qkv, qkv, qkv, d_out, out, lse)


def ln_stats(rows_in):
    rows = rows_in.astype(F32)
    mean = jnp.mean(rows, axis=-1, keepdims=True)
    centered = rows - mean
    inv = lax.rsqrt(jnp.mean(centered * centered, axis=-1, keepdims=True) + EPSILON)
    return centered * inv, inv


def layer_norm(rows_in, gain, shift):
    scaled, _ = ln_stats(rows_in)
    return (scaled * gain.astype(F32) + shift.astype(F32)).astype(BF16)


def layer_norm_bwd(rows_in, gain, d_out):
    scaled, inv = ln_stats(rows_in)
    d_out = d_out.astype(F32)
    d_scaled = d_out * gain.astype(F32)
    mean_d = jnp.mean(d_scaled, axis=-1, keepdims=True)
    mean_ds = jnp.mean(d_scaled * scaled, axis=-1, keepdims=True)
    d_rows = (inv * (d_scaled - mean_d - scaled * mean_ds)).astype(BF16)
    return d_rows, jnp.sum(d_out * scaled, axis=0), jnp.sum(d_out, axis=0)


GELU_C = 0.7978845608028654
GELU_A = 0.044715


def gelu(x):
    return 0.5 * x * (1.0 + jnp.tanh(GELU_C * (x + GELU_A * x * x * x)))


def gelu_grad(x):
    t = jnp.tanh(GELU_C * (x + GELU_A * x * x * x))
    return 0.5 * (1.0 + t) + 0.5 * x * (1.0 - t * t) * GELU_C * (1.0 + 3.0 * GELU_A * x * x)


def layer_forward(h, w, batch):
    w_qkv, w_attn, w_fc, w_proj, b_qkv, b_fc, vec = w
    a = layer_norm(h, vec[0], vec[1])
    qkv = (mm(a, w_qkv, NT) + b_qkv.astype(F32)).astype(BF16)
    o, lse = attn_fwd(qkv, batch)
    h1 = (h.astype(F32) + mm(o, w_attn, NN) + vec[2].astype(F32)).astype(BF16)
    a2 = layer_norm(h1, vec[3], vec[4])
    u = gelu(mm(a2, w_fc, NN) + b_fc.astype(F32)).astype(BF16)
    h2 = (h1.astype(F32) + mm(u, w_proj, NN) + vec[5].astype(F32)).astype(BF16)
    return h2, (h, a, qkv, o, lse, h1, a2, u)


def layer_backward(dh2, saved, w, batch):
    h, a, qkv, o, lse, h1, a2, u = saved
    w_qkv, w_attn, w_fc, w_proj, b_qkv, b_fc, vec = w
    dh2_f = dh2.astype(F32)
    d_proj = mm(u, dh2, TN).astype(BF16)
    d_b2 = jnp.sum(dh2_f, axis=0)
    du = mm(dh2, w_proj, NT).astype(BF16)
    pre = mm(lax.optimization_barrier(a2), w_fc, NN) + b_fc.astype(F32)
    d_pre = du.astype(F32) * gelu_grad(pre)
    d_bfc = jnp.sum(d_pre, axis=0)
    d_pre = d_pre.astype(BF16)
    d_fc = mm(a2, d_pre, TN).astype(BF16)
    da2 = mm(d_pre, w_fc, NT).astype(BF16)
    dh1_ln, d_g2, d_s2 = layer_norm_bwd(h1, vec[3], da2)
    dh1 = (dh1_ln.astype(F32) + dh2_f).astype(BF16)
    d_bo = jnp.sum(dh1.astype(F32), axis=0)
    d_attn = mm(o, dh1, TN).astype(BF16)
    do = mm(dh1, w_attn, NT).astype(BF16)
    dqkv = attn_bwd(qkv, do, o, lse, batch)
    d_bqkv = jnp.sum(dqkv.astype(F32), axis=1).reshape(-1)
    d_qkv = jnp.concatenate([mm(dqkv[t], a, TN).astype(BF16) for t in range(3)], axis=0)
    w3 = w_qkv.reshape(3, -1, w_qkv.shape[-1])
    da = (mm(dqkv[0], w3[0], NN) + mm(dqkv[1], w3[1], NN) + mm(dqkv[2], w3[2], NN)).astype(BF16)
    dh_ln, d_g1, d_s1 = layer_norm_bwd(h, vec[0], da)
    dh = (dh_ln.astype(F32) + dh1.astype(F32)).astype(BF16)
    small = jnp.concatenate([d_bqkv, d_bfc, d_g1, d_s1, d_bo, d_g2, d_s2, d_b2]).astype(BF16)
    return dh, (d_qkv, d_attn, d_fc, d_proj), small


def combine_body(flags_ref, *refs):
    a = refs[0:4]
    b = refs[4:8]
    out_ref = refs[-1]

    def total(parts):
        return (parts[0][...].astype(F32) + parts[1][...].astype(F32)) + (parts[2][...].astype(F32) + parts[3][...].astype(F32))

    @pl.when(flags_ref[0] == 1)
    def _():
        out_ref[0] = total(a)

    @pl.when(flags_ref[0] == 0)
    def _():
        out_ref[0] = total(b)


def combine(flags, outer, inner, prev):
    rows, cols = outer[0].shape
    blk = 256
    in_specs = [pl.BlockSpec((blk, cols), lambda i, f: (i * f[0], 0))] * 4 + [pl.BlockSpec((blk, cols), lambda i, f: (i * (1 - f[0]), 0))] * 4
    args = tuple(outer) + tuple(inner)
    aliases = {}
    if prev is not None:
        in_specs.append(pl.BlockSpec(memory_space=pl.ANY))
        args = args + (prev,)
        aliases = {9: 0}
    return pl.pallas_call(
        combine_body,
        grid_spec=pltpu.PrefetchScalarGridSpec(
            num_scalar_prefetch=1,
            grid=(rows // blk,),
            in_specs=in_specs,
            out_specs=pl.BlockSpec((1, blk, cols), lambda i, f: (f[1], i, 0)),
        ),
        out_shape=jax.ShapeDtypeStruct((2, rows, cols), F32),
        input_output_aliases=aliases,
        compiler_params=pltpu.CompilerParams(vmem_limit_bytes=56 * 1024 * 1024),
        cost_estimate=pl.CostEstimate(flops=rows * cols * 64, bytes_accessed=rows * cols * 12, transcendentals=0),
        name="combine",
    )(flags, *args)


def solution(mesh):
    n_dev = mesh.shape['pp']
    n_layers = n_dev
    data_spec = P(('dp', 'pp'))
    weight_spec = P('pp')
    swap = [(0, 1), (1, 0), (2, 3), (3, 2)]
    routes_outer = ([(1, 0), (2, 3)], [(0, 3), (3, 0)], [(2, 0), (1, 3)])
    routes_inner = ([(0, 1), (3, 2)], [(1, 2), (2, 1)], [(3, 1), (0, 2)])

    def per_device(x_loc, dy_loc, w_qkv, w_attn, w_fc, w_proj, b_qkv, b_fc, vec_d):
        pos = lax.axis_index('pp')
        upper = (pos >= 2).astype(jnp.int32)
        outer_dev = ((pos == 0) | (pos == 3)).astype(jnp.int32)
        _, batch, seq, width = x_loc.shape
        tokens = batch * seq
        own = (
            jnp.transpose(w_qkv, (0, 1, 2, 4, 5, 6, 3)).reshape(2, 3 * width, width),
            w_attn.reshape(2, width, width),
            w_fc.reshape(2, width, -1),
            w_proj.reshape(2, -1, width),
            b_qkv.reshape(2, -1),
            b_fc.reshape(2, -1),
            vec_d.reshape(2, 6, width),
        )
        peer = tuple(lax.ppermute(t, 'pp', swap) for t in own)

        def layer_weights(layer):
            copy = upper if layer < 2 else 1 - upper
            mine = outer_dev if layer in (0, 3) else 1 - outer_dev
            return tuple(
                jnp.where(mine == 1, lax.dynamic_index_in_dim(o, copy, 0, False), lax.dynamic_index_in_dim(r, copy, 0, False))
                for o, r in zip(own, peer)
            )

        weights = [layer_weights(layer) for layer in range(n_layers)]
        h = x_loc.reshape(tokens, width)
        saved = []
        for layer in range(n_layers):
            h, keep = layer_forward(h, weights[layer], batch)
            saved.append(keep)
        y = h
        d = dy_loc.reshape(tokens, width)
        parts = [None] * n_layers
        smalls = [None] * n_layers
        for layer in reversed(range(n_layers)):
            d, big, smalls[layer] = layer_backward(d, saved[layer], weights[layer], batch)
            routes = routes_outer if layer in (0, 3) else routes_inner
            parts[layer] = [(g,) + tuple(lax.ppermute(g, 'pp', r) for r in routes) for g in big]
        dx = d
        flags_hi = jnp.stack([outer_dev, 1 - upper])
        flags_lo = jnp.stack([outer_dev, upper])
        bigs = []
        for idx in range(4):
            out = combine(flags_hi, parts[3][idx], parts[2][idx], None)
            bigs.append(combine(flags_lo, parts[0][idx], parts[1][idx], out))
        gathered = lax.all_gather(jnp.stack(smalls), 'pp').astype(F32)
        total = (gathered[0] + gathered[1]) + (gathered[2] + gathered[3])
        small = jnp.stack([lax.dynamic_index_in_dim(total, pos, 0, False), lax.dynamic_index_in_dim(total, n_layers - 1 - pos, 0, False)])
        n_qkv, n_fc = 3 * width, w_fc.shape[-1]
        g_bqkv = small[:, :n_qkv].reshape((1,) + b_qkv.shape[1:])
        g_bfc = small[:, n_qkv:n_qkv + n_fc].reshape((1,) + b_fc.shape[1:])
        g_vec = small[:, n_qkv + n_fc:].reshape((1,) + vec_d.shape[1:])
        g_qkv = jnp.transpose(bigs[0].reshape(1, 2, 1, 3, HEADS, HEAD, width), (0, 1, 2, 6, 3, 4, 5))
        g_attn = bigs[1].reshape((1,) + w_attn.shape[1:])
        g_fc = bigs[2].reshape((1,) + w_fc.shape[1:])
        g_proj = bigs[3].reshape((1,) + w_proj.shape[1:])
        return (y.reshape(x_loc.shape), dx.reshape(x_loc.shape), g_qkv, g_attn, g_fc, g_proj, g_bqkv, g_bfc, g_vec)

    return jax.shard_map(per_device, mesh=mesh, in_specs=(data_spec, data_spec) + (weight_spec,) * 7, out_specs=(data_spec,) * 9, check_vma=False)
```

```python
import functools

import jax
import jax.numpy as jnp
from jax import lax
from jax.experimental import pallas as pl
from jax.experimental.pallas import tpu as pltpu
from jax.sharding import PartitionSpec as P

EPSILON = 1e-5
HEADS = 12
HEAD = 64
LANES = 128
WIDTH = HEADS * HEAD
PAIRS = WIDTH // LANES
LOG2E = 1.4426950408889634
SCALE = HEAD ** -0.5
EXP_SCALE = SCALE * LOG2E
BLK = 256
ROWS = 512
HALF = WIDTH // 2
FOUR = 4
N_STAT = 16
GELU_C = 0.7978845608028654
GELU_A = 0.044715
GELU_CA = GELU_C * GELU_A
ROW_FC, ROW_G1, ROW_S1, ROW_BO, ROW_G2, ROW_S2, ROW_B2 = 3, 7, 8, 9, 10, 11, 12
VMEM_LIMIT = 60 * 1024 * 1024
F32 = jnp.float32
BF16 = jnp.bfloat16
NT = (((1,), (1,)), ((), ()))
NN = (((1,), (0,)), ((), ()))
TN = (((0,), (0,)), ((), ()))
ANY = pl.BlockSpec(memory_space=pl.ANY)
MESH_ID = pl.DeviceIdType.MESH


def mm(a, b, dims):
    return lax.dot_general(a, b, dims, preferred_element_type=F32)


def iota(shape, dim):
    return lax.broadcasted_iota(jnp.int32, shape, dim)


def row_max(x):
    return jnp.max(x, axis=-1, keepdims=True)


def row_sum(x):
    return jnp.sum(x, axis=-1, keepdims=True)


def col_sum(x):
    return jnp.sum(x, axis=0, keepdims=True)


def row_mean(x):
    return jnp.mean(x, axis=-1, keepdims=True)


def chunk(index):
    return slice(index * WIDTH, (index + 1) * WIDTH)


def lanes_of(index):
    return pl.ds(pl.multiple_of(index * LANES, LANES), LANES)


def rows_of(index):
    return pl.ds(pl.multiple_of(index * ROWS, ROWS), ROWS)


def stat_row(s_ref, row):
    return s_ref[0, row : row + 1]


def ln_parts(rows_in):
    rows = rows_in.astype(F32)
    centered = rows - row_mean(rows)
    inv = lax.rsqrt(row_mean(centered * centered) + EPSILON)
    return centered * inv, inv


def ln_apply(rows_in, gain, shift):
    scaled, _ = ln_parts(rows_in)
    return (scaled * gain + shift).astype(BF16)


def ln_grad(rows_in, gain, d_out):
    scaled, inv = ln_parts(rows_in)
    d_scaled = d_out * gain
    d_rows = (inv * (d_scaled - row_mean(d_scaled) - scaled * row_mean(d_scaled * scaled))).astype(BF16)
    return d_rows, col_sum(d_out * scaled), col_sum(d_out)


def gelu_terms(pre):
    square = pre * pre
    t = jnp.tanh(pre * (GELU_C + GELU_CA * square))
    return square, t, 0.5 + 0.5 * t


def start_load(flags_ref, layer, pair, dst, sem):
    own_ref, peer_ref = pair

    @pl.when(flags_ref[layer, 0] == 1)
    def _():
        pltpu.make_async_copy(own_ref.at[flags_ref[layer, 1]], dst, sem).start()

    @pl.when(flags_ref[layer, 0] == 0)
    def _():
        pltpu.make_async_copy(peer_ref.at[flags_ref[layer, 1]], dst, sem).start()


def wait_load(pair, dst, sem):
    pltpu.make_async_copy(pair[0].at[0], dst, sem).wait()


def attend(qkv_ref, o_ref, lse_scr, pair, seq):
    lane = iota((BLK, LANES), 1)
    causal = iota((BLK, BLK), 0) >= iota((BLK, BLK), 1)
    q_at, k_at, v_at = (lanes_of(t * PAIRS + pair) for t in range(3))
    zero = jnp.zeros((BLK, LANES), BF16)
    for i in range(seq // BLK):
        past, rows = slice(0, i * BLK), slice(i * BLK, (i + 1) * BLK)
        q_blk = qkv_ref[rows, q_at]
        heads_out = []
        stats = lse_scr[rows, :]
        for h in range(2):
            q_h = jnp.where((lane < HEAD) == (h == 0), q_blk, zero)
            s_d = jnp.where(causal, mm(q_h, qkv_ref[rows, k_at], NT), -1e30)
            top = row_max(s_d)
            if i:
                s_o = mm(q_h, qkv_ref[past, k_at], NT)
                top = jnp.maximum(top, row_max(s_o))
            e_d = jnp.exp2((s_d - top) * EXP_SCALE)
            total = row_sum(e_d)
            if i:
                e_o = jnp.exp2((s_o - top) * EXP_SCALE)
                total = total + row_sum(e_o)
            inv = 1.0 / total
            out = mm((e_d * inv).astype(BF16), qkv_ref[rows, v_at], NN)
            if i:
                out = out + mm((e_o * inv).astype(BF16), qkv_ref[past, v_at], NN)
            heads_out.append(out)
            stats = jnp.where(lane == 2 * pair + h, top * EXP_SCALE + jnp.log2(total), stats)
        o_ref[rows, lanes_of(pair)] = jnp.where(lane < HEAD, *heads_out).astype(BF16)
        lse_scr[rows, :] = stats


def forward_body(keep_u, flags_ref, x_ref, s_ref, *refs):
    weights = [refs[2 * k : 2 * k + 2] for k in range(FOUR)]
    n_out = 7 + keep_u
    outs = refs[2 * FOUR : 2 * FOUR + n_out]
    w_bufs = refs[2 * FOUR + n_out : 3 * FOUR + n_out]
    h_scr, a_scr, qkv_scr, o_scr, lse_scr, lse_t, h1_scr, a2_scr, w_sems, out_sems, x_sem = refs[3 * FOUR + n_out : 3 * FOUR + n_out + 11]
    u_scr = refs[-1] if keep_u else None
    layer = pl.program_id(0)
    n_layers = pl.num_programs(0)
    slot = layer % 2
    seq = x_ref.shape[0]
    w_q, w_o, w_1, w_2 = (w.at[slot] for w in w_bufs)

    def saves(at, h_slot):
        sources = [h_scr.at[h_slot], a_scr, qkv_scr, o_scr, lse_t, h1_scr, a2_scr]
        return [pltpu.make_async_copy(src, out.at[at], out_sems.at[k]) for k, (src, out) in enumerate(zip(sources, outs))]

    def load(at, to):
        for k in range(FOUR):
            start_load(flags_ref, at, weights[k], w_bufs[k].at[to], w_sems.at[to, k])

    @pl.when(layer == 0)
    def _():
        load(0, 0)
        first = pltpu.make_async_copy(x_ref, h_scr.at[0], x_sem)
        first.start()
        first.wait()

    @pl.when(layer + 1 < n_layers)
    def _():
        load(layer + 1, 1 - slot)

    def finish(index):
        @pl.when(layer > 0)
        def _():
            saves(layer - 1, slot)[index].wait()

    wait_load(weights[0], w_q, w_sems.at[slot, 0])
    finish(1)
    finish(2)

    @pl.loop(0, seq // ROWS)
    def _(block):
        rows = rows_of(block)
        a = ln_apply(h_scr[slot, rows, :], stat_row(s_ref, ROW_G1), stat_row(s_ref, ROW_S1))
        a_scr[rows, :] = a
        for t in range(3):
            qkv_scr[rows, chunk(t)] = (mm(a, w_q[chunk(t), :], NT) + stat_row(s_ref, t)).astype(BF16)

    now = saves(layer, 1 - slot)
    now[1].start()
    now[2].start()
    finish(3)
    finish(4)
    lse_scr[...] = jnp.zeros_like(lse_scr)

    @pl.loop(0, PAIRS)
    def _(pair):
        attend(qkv_scr, o_scr, lse_scr, pair, seq)

    lse_t[...] = lse_scr[...].T[:N_STAT, :]
    now[3].start()
    now[4].start()
    for k in range(1, FOUR):
        wait_load(weights[k], (w_q, w_o, w_1, w_2)[k], w_sems.at[slot, k])
    finish(5)
    finish(6)
    finish(0)

    @pl.loop(0, seq // ROWS)
    def _(block):
        rows = rows_of(block)
        h1 = (h_scr[slot, rows, :].astype(F32) + mm(o_scr[rows, :], w_o[...], NN) + stat_row(s_ref, ROW_BO)).astype(BF16)
        h1_scr[rows, :] = h1
        a2 = ln_apply(h1, stat_row(s_ref, ROW_G2), stat_row(s_ref, ROW_S2))
        a2_scr[rows, :] = a2
        acc = stat_row(s_ref, ROW_B2)
        for j in range(w_1.shape[1] // WIDTH):
            pre = mm(a2, w_1[:, chunk(j)], NN) + stat_row(s_ref, ROW_FC + j)
            _, _, half = gelu_terms(pre)
            u = (pre * half).astype(BF16)
            if keep_u:
                u_scr[rows, chunk(j)] = u
            acc = acc + mm(u, w_2[chunk(j), :], NN)
        h_scr[1 - slot, rows, :] = (h1.astype(F32) + acc).astype(BF16)

    now[5].start()
    now[6].start()
    now[0].start()

    @pl.when(layer == n_layers - 1)
    def _():
        if keep_u:
            extra = pltpu.make_async_copy(u_scr, outs[-1], x_sem)
            extra.start()
            extra.wait()
        for copy in now:
            copy.wait()


def forward_stack(x, flags, small, weights, keep_u):
    seq = x.shape[0]
    n_layers = small.shape[0]
    n_fc = weights[2][0].shape[-1]
    stack = lambda cols: jax.ShapeDtypeStruct((n_layers, seq, cols), BF16)
    out_shape = [stack(WIDTH), stack(WIDTH), stack(3 * WIDTH), stack(WIDTH), jax.ShapeDtypeStruct((n_layers, N_STAT, seq), F32), stack(WIDTH), stack(WIDTH)]
    act = lambda cols: pltpu.VMEM((seq, cols), BF16)
    scratch = [pltpu.VMEM((2,) + own.shape[1:], BF16) for own, _ in weights]
    scratch += [pltpu.VMEM((2, seq, WIDTH), BF16), act(WIDTH), act(3 * WIDTH), act(WIDTH), pltpu.VMEM((seq, LANES), F32), pltpu.VMEM((N_STAT, seq), F32), act(WIDTH), act(WIDTH)]
    scratch += [pltpu.SemaphoreType.DMA((2, FOUR)), pltpu.SemaphoreType.DMA((7,)), pltpu.SemaphoreType.DMA]
    if keep_u:
        out_shape.append(jax.ShapeDtypeStruct((seq, n_fc), BF16))
        scratch.append(act(n_fc))
    flat = [w for pair in weights for w in pair]
    return pl.pallas_call(
        functools.partial(forward_body, keep_u),
        grid_spec=pltpu.PrefetchScalarGridSpec(
            num_scalar_prefetch=1,
            grid=(n_layers,),
            in_specs=[ANY, pl.BlockSpec((1,) + small.shape[1:], lambda l, f: (l, 0, 0))] + [ANY] * len(flat),
            out_specs=[ANY] * len(out_shape),
            scratch_shapes=scratch,
        ),
        out_shape=out_shape,
        compiler_params=pltpu.CompilerParams(vmem_limit_bytes=VMEM_LIMIT),
        cost_estimate=pl.CostEstimate(flops=n_layers * seq * WIDTH * (HEADS * WIDTH + FOUR * n_fc), bytes_accessed=n_layers * seq * WIDTH * HEADS, transcendentals=0),
        name="forward_stack",
    )(flags, x, small, *flat)


def picked_spec(block, index_map, picked):
    _, at = picked
    if at is None:
        return pl.BlockSpec(block, index_map)
    return pl.BlockSpec((None,) + block, lambda *ids: (at,) + index_map(*ids))


def attn_bwd_body(q_ref, k_ref, v_ref, do_ref, o_ref, lse_ref, dqkv_hbm, db_ref, dq_scr, delta_scr, stage, sems):
    pair = pl.program_id(0)
    last = pl.num_programs(0) - 1
    slot = pair % 2
    seq = q_ref.shape[0]
    n_blk = seq // BLK
    lane = iota((seq, LANES), 1)
    first = lane < HEAD

    def copies(at_pair, at_slot):
        return [pltpu.make_async_copy(stage.at[at_slot, t], dqkv_hbm.at[:, lanes_of(t * PAIRS + at_pair)], sems.at[at_slot, t]) for t in range(3)]

    @pl.when(pair >= 2)
    def _():
        for copy in copies(pair - 2, slot):
            copy.wait()

    causal_t = iota((BLK, BLK), 0) <= iota((BLK, BLK), 1)
    prod = do_ref[...].astype(F32) * o_ref[...].astype(F32)
    halves = lambda x: (jnp.where(first, x, jnp.zeros_like(x)), jnp.where(first, jnp.zeros_like(x), x))
    delta_scr[...] = jnp.where(lane == 0, *(row_sum(p) for p in halves(prod))).T[: delta_scr.shape[0], :]
    q_h, do_h, k_h = (halves(ref[...]) for ref in (q_ref, do_ref, k_ref))
    dq_scr[...] = jnp.zeros_like(dq_scr)
    sum_k = sum_v = jnp.zeros((1, LANES), F32)
    for j in range(n_blk):
        keys, rest = slice(j * BLK, (j + 1) * BLK), slice((j + 1) * BLK, seq)
        k_blk, v_blk = k_ref[keys, :], v_ref[keys, :]
        dk = dv = jnp.zeros((BLK, LANES), F32)
        for h in range(2):
            for rows in (keys, rest)[: 1 + (j + 1 < n_blk)]:
                q_p, do_p = q_h[h][rows], do_h[h][rows]
                lse = lse_ref[pl.ds(2 * pair + h, 1), rows]
                p_t = jnp.exp2(mm(k_blk, q_p, NT) * EXP_SCALE - lse)
                if rows is keys:
                    p_t = jnp.where(causal_t, p_t, 0.0)
                ds_t = (p_t * (mm(v_blk, do_p, NT) - delta_scr[h : h + 1, rows])).astype(BF16)
                dv = dv + mm(p_t.astype(BF16), do_p, NN)
                dk = dk + mm(ds_t, q_p, NN)
                dq_scr[rows, :] += mm(ds_t, k_h[h][keys], TN)
        dk, dv = (dk * SCALE).astype(BF16), dv.astype(BF16)
        stage[slot, 1, keys, :] = dk
        stage[slot, 2, keys, :] = dv
        sum_k, sum_v = sum_k + col_sum(dk.astype(F32)), sum_v + col_sum(dv.astype(F32))
    dq = (dq_scr[...] * SCALE).astype(BF16)
    stage[slot, 0] = dq
    for t, total in enumerate((col_sum(dq.astype(F32)), sum_k, sum_v)):
        db_ref[t] = jnp.broadcast_to(total, db_ref.shape[1:])
    for copy in copies(pair, slot):
        copy.start()

    @pl.when(pair == last)
    def _():
        for copy in copies(pair - 1, 1 - slot) + copies(pair, slot):
            copy.wait()


def attn_bwd(qkv, d_out, out, lse):
    seq = d_out.shape[0]
    block = (seq, LANES)
    column = lambda t: (lambda p: (0, t * PAIRS + p))
    return pl.pallas_call(
        attn_bwd_body,
        grid=(PAIRS,),
        in_specs=[picked_spec(block, column(t), qkv) for t in range(3)]
        + [pl.BlockSpec(block, column(0)), picked_spec(block, column(0), out), picked_spec((N_STAT, seq), lambda p: (0, 0), lse)],
        out_specs=[ANY, pl.BlockSpec((3, N_STAT, LANES), lambda p: (0, 0, p))],
        out_shape=[jax.ShapeDtypeStruct((seq, 3 * WIDTH), BF16), jax.ShapeDtypeStruct((3, N_STAT, WIDTH), F32)],
        scratch_shapes=[pltpu.VMEM(block, F32), pltpu.VMEM((N_STAT, seq), F32), pltpu.VMEM((2, 3) + block, BF16), pltpu.SemaphoreType.DMA((2, 3))],
        compiler_params=pltpu.CompilerParams(vmem_limit_bytes=VMEM_LIMIT),
        cost_estimate=pl.CostEstimate(flops=FOUR * FOUR * seq * seq * WIDTH, bytes_accessed=N_STAT * seq * WIDTH, transcendentals=0),
        name="attn_bwd",
    )(qkv[0], qkv[0], qkv[0], d_out, out[0], lse[0])


def row_call(body, layer, flags, rows_in, small, weights, out_cols, flops):
    tokens = rows_in[0][0].shape[-2]
    index_map = lambda i, f: (i, 0)
    in_specs = [picked_spec((ROWS, r[0].shape[-1]), index_map, r) for r in rows_in]
    in_specs.append(pl.BlockSpec((1,) + small.shape[1:], lambda i, f: (layer, 0, 0)))
    flat = [w for pair in weights for w in pair]
    return pl.pallas_call(
        functools.partial(body, layer),
        grid_spec=pltpu.PrefetchScalarGridSpec(
            num_scalar_prefetch=1,
            grid=(tokens // ROWS,),
            in_specs=in_specs + [ANY] * len(flat),
            out_specs=[pl.BlockSpec((ROWS, c), index_map) for c in out_cols] + [pl.BlockSpec((N_STAT, WIDTH), lambda i, f: (0, 0))],
            scratch_shapes=[pltpu.VMEM(own.shape[1:], BF16) for own, _ in weights] + [pltpu.SemaphoreType.DMA((len(weights),))],
        ),
        out_shape=[jax.ShapeDtypeStruct((tokens, c), BF16) for c in out_cols] + [jax.ShapeDtypeStruct((N_STAT, WIDTH), F32)],
        compiler_params=pltpu.CompilerParams(vmem_limit_bytes=VMEM_LIMIT),
        cost_estimate=pl.CostEstimate(flops=flops, bytes_accessed=tokens * sum(out_cols) * FOUR, transcendentals=0),
    )(flags, *(r for r, _ in rows_in), small, *flat)


def load_all(layer, flags_ref, sums_ref, pairs, bufs, sem):
    @pl.when(pl.program_id(0) == 0)
    def _():
        sums_ref[...] = jnp.zeros_like(sums_ref)
        for k, (pair, buf) in enumerate(zip(pairs, bufs)):
            start_load(flags_ref, layer, pair, buf, sem.at[k])
        for k, (pair, buf) in enumerate(zip(pairs, bufs)):
            wait_load(pair, buf, sem.at[k])


def mlp_bwd_body(save_u, layer, flags_ref, dh2_ref, a2_ref, h1_ref, s_ref, *refs):
    pairs = [refs[2 * k : 2 * k + 2] for k in range(3)]
    dpre_ref, dh1_ref, do_ref = refs[6:9]
    sums_ref, w_o, w_1, w_2, sem = refs[-5:]
    load_all(layer, flags_ref, sums_ref, pairs, (w_o, w_1, w_2), sem)

    def add_sum(row, value):
        sums_ref[row : row + 1, :] += value

    dh2 = dh2_ref[...]
    a2 = a2_ref[...]
    da2 = None
    for j in range(w_1.shape[1] // WIDTH):
        du = mm(dh2, w_2[chunk(j), :], NT).astype(BF16).astype(F32)
        pre = mm(a2, w_1[:, chunk(j)], NN) + stat_row(s_ref, ROW_FC + j)
        square, t, half = gelu_terms(pre)
        if save_u:
            refs[9][:, chunk(j)] = (pre * half).astype(BF16)
        slope = half + (0.5 * pre) * (1.0 - t * t) * (GELU_C + (3.0 * GELU_CA) * square)
        d_pre = du * slope
        add_sum(ROW_FC + j, col_sum(d_pre))
        d_pre = d_pre.astype(BF16)
        dpre_ref[:, chunk(j)] = d_pre
        part = mm(d_pre, w_1[:, chunk(j)], NT)
        da2 = part if da2 is None else da2 + part
    d_rows, d_gain, d_shift = ln_grad(h1_ref[...], stat_row(s_ref, ROW_G2), da2.astype(BF16).astype(F32))
    dh2_f = dh2.astype(F32)
    dh1 = (d_rows.astype(F32) + dh2_f).astype(BF16)
    dh1_ref[...] = dh1
    add_sum(ROW_BO, col_sum(dh1.astype(F32)))
    add_sum(ROW_G2, d_gain)
    add_sum(ROW_S2, d_shift)
    add_sum(ROW_B2, col_sum(dh2_f))
    do_ref[...] = mm(dh1, w_o[...], NT).astype(BF16)


def qkv_bwd_body(layer, flags_ref, dqkv_ref, h_ref, dh1_ref, s_ref, own_ref, peer_ref, dh_ref, sums_ref, w_q, sem):
    load_all(layer, flags_ref, sums_ref, [(own_ref, peer_ref)], [w_q], sem)
    da = mm(dqkv_ref[...], w_q[...], NN).astype(BF16).astype(F32)
    d_rows, d_gain, d_shift = ln_grad(h_ref[...], stat_row(s_ref, ROW_G1), da)
    dh_ref[...] = (d_rows.astype(F32) + dh1_ref[...].astype(F32)).astype(BF16)
    sums_ref[ROW_G1 : ROW_G1 + 1, :] += d_gain
    sums_ref[ROW_S1 : ROW_S1 + 1, :] += d_shift


def wgrad_body(plan, *refs):
    n_pair = len(plan)
    lhs_refs = refs[0 : 2 * n_pair : 2]
    rhs_refs = refs[1 : 2 * n_pair : 2]
    out_ref, send_buf, recv_buf, send_sems, recv_sems = refs[2 * n_pair :]
    pos = lax.axis_index("pp")
    core = pos % 2
    partner = {"pp": pos + 1 - 2 * core}
    barrier = pltpu.get_barrier_semaphore()
    pl.semaphore_signal(barrier, device_id=partner, device_id_type=MESH_ID)
    pl.semaphore_wait(barrier)

    def copy(tile):
        return pltpu.make_async_remote_copy(send_buf.at[tile], recv_buf.at[tile], send_sems.at[tile], recv_sems.at[tile], device_id=partner, device_id_type=MESH_ID)

    def product(index, tile, half):
        unit, col = (tile, 0) if plan[index][1] == 1 else (0, tile)
        lhs = lhs_refs[index][:, pl.ds(pl.multiple_of(unit * WIDTH + half * HALF, LANES), HALF)]
        rhs = rhs_refs[index][:, pl.ds(pl.multiple_of(col * WIDTH, LANES), WIDTH)]
        return mm(lhs, rhs, TN)

    counts = [units * cols for units, cols in plan]
    starts = [sum(counts[:index]) for index in range(n_pair)]
    total = sum(counts)
    for index in range(n_pair):

        @pl.loop(0, counts[index])
        def _(tile, index=index, base=starts[index]):
            send_buf[base + tile] = product(index, tile, 1 - core)

            @pl.when(base + tile > 0)
            def _():
                copy(base + tile - 1).start()

    for index in range(n_pair):

        @pl.loop(0, counts[index])
        def _(tile, index=index, base=starts[index]):
            mine = product(index, tile, core)

            @pl.when(base + tile == 0)
            def _():
                copy(total - 1).start()

            copy(base + tile).wait_recv()
            out_ref[base + tile] = (mine + recv_buf[base + tile]).astype(BF16)

    @pl.loop(0, total)
    def _(tile):
        copy(tile).wait_send()


def wgrad(pairs, collective_id):
    flat = [side for pair in pairs for side in pair]
    plan = tuple((lhs[0].shape[-1] // WIDTH, rhs[0].shape[-1] // WIDTH) for lhs, rhs in pairs)
    total = sum(u * c for u, c in plan)
    seq = flat[0][0].shape[-2]
    return pl.pallas_call(
        functools.partial(wgrad_body, plan),
        grid=(1,),
        in_specs=[picked_spec((seq, side[0].shape[-1]), lambda i: (0, 0), side) for side in flat],
        out_specs=pl.BlockSpec((total, HALF, WIDTH), lambda i: (0, 0, 0)),
        out_shape=jax.ShapeDtypeStruct((total, HALF, WIDTH), BF16),
        scratch_shapes=[pltpu.VMEM((total, HALF, WIDTH), F32)] * 2 + [pltpu.SemaphoreType.DMA((total,))] * 2,
        compiler_params=pltpu.CompilerParams(collective_id=collective_id, has_side_effects=True, vmem_limit_bytes=VMEM_LIMIT),
        cost_estimate=pl.CostEstimate(flops=2 * total * seq * WIDTH * WIDTH, bytes_accessed=total * FOUR * WIDTH * WIDTH, transcendentals=0),
    )(*(side[0] for side in flat))


def layer_backward(dh2, saved, w, layer, exchange):
    h, a, qkv, o, lse, h1, a2, u = saved
    flags, small, w_qkv, w_attn, w_fc, w_proj = w
    tokens, n_fc = dh2.shape[0], w_fc[0].shape[-1]
    split = u is not None
    own, received = [], []

    def send(pairs, collective_id, follow):
        g = wgrad(pairs, collective_id)
        follow, g = lax.optimization_barrier((follow, g))
        received.append(exchange(g))
        own.append(g)
        return follow

    whole = lambda x: (x, None)
    if split:
        dh2 = send([(whole(u), whole(dh2))], 1, dh2)
    outs = row_call(
        functools.partial(mlp_bwd_body, not split), layer, flags, [whole(dh2), a2, h1], small, [w_attn, w_fc, w_proj],
        [n_fc, WIDTH, WIDTH] + [n_fc] * (not split), 2 * tokens * WIDTH * (WIDTH + 3 * n_fc),
    )
    d_pre, dh1, do, sums = outs[0], outs[1], outs[2], outs[-1]
    pair_fc = (a2, whole(d_pre))
    if split:
        do = send([pair_fc], 2, do)
    else:
        do = send([(whole(outs[3]), whole(dh2)), pair_fc], 3, do)
    dqkv, d_bqkv = attn_bwd(qkv, do, o, lse)
    dqkv = send([(whole(dqkv), a), (o, whole(dh1))], FOUR, dqkv)
    dh, sums_q = row_call(qkv_bwd_body, layer, flags, [whole(dqkv), h, whole(dh1)], small, [w_qkv], [WIDTH], 6 * tokens * WIDTH * WIDTH)
    small_grads = jnp.concatenate([d_bqkv[:, 0], sums[ROW_FC:ROW_G1], sums_q[ROW_G1:ROW_BO], sums[ROW_BO : ROW_B2 + 1]], axis=0)
    return dh, own, received, small_grads


def total_of(parts):
    a, b, c, d = (p[0].astype(F32) for p in parts)
    return (a + b) + (c + d)


def part_specs(parts, blk, index_of):
    return [pl.BlockSpec(blk, functools.partial(index_of, off)) for _, off in parts]


def send_total_body(flags_ref, *refs):
    out_ref = refs[-1]
    for flag in range(2):

        @pl.when(flags_ref[0] == flag)
        def _(flag=flag):
            out_ref[0] = total_of(refs[FOUR * flag : FOUR * (flag + 1)])


def send_total(flags, outer, inner):
    blk = (1, HALF, WIDTH)
    return pl.pallas_call(
        send_total_body,
        grid_spec=pltpu.PrefetchScalarGridSpec(
            num_scalar_prefetch=1,
            grid=(FOUR,),
            in_specs=part_specs(outer, blk, lambda off, i, f: (off + i * (1 - f[0]), 0, 0)) + part_specs(inner, blk, lambda off, i, f: (off + i * f[0], 0, 0)),
            out_specs=pl.BlockSpec(blk, lambda i, f: (i, 0, 0)),
        ),
        out_shape=jax.ShapeDtypeStruct((FOUR, HALF, WIDTH), F32),
        cost_estimate=pl.CostEstimate(flops=HALF * WIDTH * BLK, bytes_accessed=HALF * WIDTH * FOUR * HEADS, transcendentals=0),
        name="send_total",
    )(flags, *(p for p, _ in outer + inner))


def final_total_body(flags_ref, *refs):
    recv_ref, out_ref = refs[2 * FOUR], refs[-1]
    mine = pl.program_id(1) == flags_ref[2]
    for flag in range(2):

        @pl.when(mine & (flags_ref[0] == 1 - flag))
        def _(flag=flag):
            out_ref[0] = total_of(refs[FOUR * flag : FOUR * (flag + 1)])

    @pl.when(jnp.logical_not(mine))
    def _():
        out_ref[0] = recv_ref[0]


def final_total(flags, outer, inner, recv, first, count, by_rows, prev):
    blk = (1, HALF, WIDTH)
    in_specs = part_specs(outer, blk, lambda off, i, h, f: (off + i * f[0], 0, 0)) + part_specs(inner, blk, lambda off, i, h, f: (off + i * (1 - f[0]), 0, 0))
    in_specs.append(pl.BlockSpec(blk, lambda i, h, f: (first + i, 0, 0)))
    args = [p for p, _ in outer + inner] + [recv]
    aliases = {}
    if prev is not None:
        in_specs.append(ANY)
        args.append(prev)
        aliases = {len(args): 0}
    long, wide = (count, 1) if by_rows else (1, count)
    out_map = (lambda i, h, f: (f[1], 2 * i + h, 0)) if by_rows else (lambda i, h, f: (f[1], h, i))
    return pl.pallas_call(
        final_total_body,
        grid_spec=pltpu.PrefetchScalarGridSpec(num_scalar_prefetch=1, grid=(count, 2), in_specs=in_specs, out_specs=pl.BlockSpec(blk, out_map)),
        out_shape=jax.ShapeDtypeStruct((2, long * WIDTH, wide * WIDTH), F32),
        input_output_aliases=aliases,
        cost_estimate=pl.CostEstimate(flops=count * HALF * WIDTH * BLK, bytes_accessed=count * WIDTH * WIDTH * HEADS, transcendentals=0),
        name="final_total",
    )(flags, *args)


def solution(mesh):
    n_layers = mesh.shape['pp']
    data_spec = P(('dp', 'pp'))
    weight_spec = P('pp')
    swap = [(i, i ^ 1) for i in range(n_layers)]
    cross = [(i, i ^ 2) for i in range(n_layers)]

    def per_device(x_loc, dy_loc, w_qkv, w_attn, w_fc, w_proj, b_qkv, b_fc, vec_d):
        pos = lax.axis_index('pp')
        core = pos % 2
        upper = pos // 2
        outer_dev = 1 - (core ^ upper)
        width, n_fc = WIDTH, w_fc.shape[-1]
        own = (
            jnp.transpose(w_qkv, (0, 1, 2, 4, 5, 6, 3)).reshape(2, 3 * width, width),
            w_attn.reshape(2, width, width),
            w_fc.reshape(2, width, n_fc),
            w_proj.reshape(2, n_fc, width),
        )
        own_small = jnp.concatenate([b_qkv.reshape(2, -1), b_fc.reshape(2, -1), vec_d.reshape(2, -1)], axis=1)
        trade = lambda t: lax.ppermute(t, 'pp', swap)
        pick = lambda t, at: lax.dynamic_index_in_dim(t, at, 0, False)

        def by_sequence(mine):
            got = trade(pick(mine, 1 - core))
            return jnp.where(core == 0, mine[0], got), jnp.where(core == 0, got, mine[1])

        def by_micro(first, second):
            got = trade(jnp.where(core == 0, second, first))
            return jnp.where(core == 0, jnp.stack([first, got]), jnp.stack([got, second]))

        xs = by_sequence(x_loc[0])
        peer_small = trade(own_small)
        peer = tuple(trade(t) for t in own)
        flags = jnp.stack([jnp.stack([outer_dev if l in (0, n_layers - 1) else 1 - outer_dev, upper if l < 2 else 1 - upper]) for l in range(n_layers)])
        small_of = lambda l: jnp.where(flags[l, 0] == 1, pick(own_small, flags[l, 1]), pick(peer_small, flags[l, 1]))
        small_w = jnp.stack([small_of(l) for l in range(n_layers)]).astype(F32).reshape(n_layers, -1, width)
        weights = tuple(zip(own, peer))
        ys, dxs, smalls = [], [], []
        parts = [[] for _ in range(n_layers)]
        dys = None
        for micro in range(2):
            x = xs[micro]
            if micro:
                x, _ = lax.optimization_barrier((x, dxs[0]))
            first = micro == 0
            res = forward_stack(x, flags, small_w, weights, first)
            if first:
                late, _ = lax.optimization_barrier((dy_loc, peer[2]))
                dys = by_sequence(late[0])
            ys.append(res[0][n_layers - 1])
            d = dys[micro]
            for layer in reversed(range(n_layers)):
                saved = [(res[0], layer - 1) if layer else (x, None)] + [(r, layer) for r in res[1:7]]
                saved.append(res[7] if first and layer == n_layers - 1 else None)
                d, sent, got, small = layer_backward(d, saved, (flags, small_w) + weights, layer, lambda g: lax.ppermute(g, 'pp', cross))
                smalls.append(small)
                parts[layer].append((sent, got))
            dxs.append(d)
        small = jnp.stack(smalls).reshape(2 * n_layers, -1)
        small = (small + trade(small)).astype(BF16)
        both = jnp.stack([small, lax.ppermute(small, 'pp', cross)]).astype(F32)
        both = both[:, :n_layers] + both[:, n_layers:]
        small = both[0] + both[1]
        small = jnp.stack([pick(small, n_layers - 1 - pos), pick(small, pos)])

        def pieces(layer, group):
            picked = []
            for which in range(2):
                for sets in parts[layer]:
                    arrays = sets[which]
                    if group == 2:
                        picked.append((arrays[-1], 0))
                    else:
                        picked.append((arrays[group], 0) if len(arrays) > 2 else (arrays[0], FOUR * group))
            return picked

        outs = [None] * FOUR
        plans = (((3, 0, FOUR, True),), ((2, 0, FOUR, False),), ((0, 0, 3, True), (1, 3, 1, True)))
        after = d
        for high in (True, False):
            outer_layer, inner_layer, copy = (3, 2, 1 - upper) if high else (0, 1, upper)
            for group, slots in enumerate(plans):
                order, _ = lax.optimization_barrier((jnp.stack([outer_dev, copy, core]), after))
                outer, inner = pieces(outer_layer, group), pieces(inner_layer, group)
                sent = send_total(order, outer, inner)
                recv = trade(sent)
                for slot, first, count, by_rows in slots:
                    shifted = [[(p, off + first) for p, off in side] for side in (outer, inner)]
                    outs[slot] = final_total(order, *shifted, recv, first, count, by_rows, outs[slot])
                after = sent if high else outs[slots[0][0]]
            if high:
                after, *outs = lax.optimization_barrier([after] + outs)
        n_qkv = 3 * width
        g_bqkv = small[:, :n_qkv].reshape((1,) + b_qkv.shape[1:])
        g_bfc = small[:, n_qkv : n_qkv + n_fc].reshape((1,) + b_fc.shape[1:])
        g_vec = small[:, n_qkv + n_fc :].reshape((1,) + vec_d.shape[1:])
        g_qkv = jnp.transpose(outs[0].reshape(1, 2, 1, 3, HEADS, HEAD, width), (0, 1, 2, 6, 3, 4, 5))
        g_attn, g_fc, g_proj = (out.reshape((1,) + t.shape[1:]) for out, t in zip(outs[1:], (w_attn, w_fc, w_proj)))
        y, dx = by_micro(*ys), by_micro(*dxs)
        return (y[None], dx[None], g_qkv, g_attn, g_fc, g_proj, g_bqkv, g_bfc, g_vec)

    return jax.shard_map(per_device, mesh=mesh, in_specs=(data_spec,) * 2 + (weight_spec,) * 7, out_specs=(data_spec,) * 9, check_vma=False)
```
